8 devices in a mesh: fsdp: 8 (over z, y, x, core).
Axes of the slice: x: 2, y: 2, z: 1, core: 2. Of those that a mesh axis runs over, the one named last changes fastest.
Arguments:
- acts_in: bfloat16 [4, 32768, 768], P(None, 'fsdp')
- cot_out: bfloat16 [4, 32768, 768], P(None, 'fsdp')
- w_in: bfloat16 [2, 768, 3072], P(None, 'fsdp')
- w_out: bfloat16 [2, 3072, 768], P(None, 'fsdp')
Outputs:
- output 1: float32 [2, 768, 3072], P(None, 'fsdp')
- output 2: float32 [2, 3072, 768], P(None, 'fsdp')
All inputs are finite; a program needn't handle non-finite values.
Results may differ from the reference program's by a relative error of at most 0.011845.
Values are sent between devices in bfloat16 or wider.
A program may use at most 1 GiB of HBM per device.

```python
import math
import jax
import jax.numpy as jnp
from jax import lax

MODEL_DIM = 768
HIDDEN_DIM = 3072
MICRO_STEPS = 4
NUM_LAYERS = 2
ALL_TOKENS = 32768
TOKEN_BLOCK = 2048


def gelu_pair(hidden):
    h_float = hidden.astype(jnp.float32)
    gelu_coeff = math.sqrt(2.0 / math.pi)
    tanh_val = jnp.tanh(gelu_coeff * (h_float + 0.044715 * h_float * h_float * h_float))
    gelu_value = 0.5 * h_float * (1.0 + tanh_val)
    gelu_slope = 0.5 * (1.0 + tanh_val) + 0.5 * h_float * (1.0 - tanh_val * tanh_val) * gelu_coeff * (1.0 + 3.0 * 0.044715 * h_float * h_float)
    return gelu_value.astype(jnp.bfloat16), gelu_slope


def setup_inputs(seed: int = 0) -> dict:
    rng_key = jax.random.key(seed)
    key_x, key_g, key_w1, key_w2 = jax.random.split(rng_key, 4)
    tok_shape = (MICRO_STEPS, ALL_TOKENS, MODEL_DIM)
    acts_in = jax.random.normal(key_x, tok_shape, jnp.float32).astype(jnp.bfloat16)
    grad_scale = (MICRO_STEPS * ALL_TOKENS) ** -0.5
    cot_out = (jax.random.normal(key_g, tok_shape, jnp.float32) * grad_scale).astype(jnp.bfloat16)
    w_in = (jax.random.normal(key_w1, (NUM_LAYERS, MODEL_DIM, HIDDEN_DIM), jnp.float32) * MODEL_DIM ** -0.5).astype(jnp.bfloat16)
    w_out = (jax.random.normal(key_w2, (NUM_LAYERS, HIDDEN_DIM, MODEL_DIM), jnp.float32) * HIDDEN_DIM ** -0.5).astype(jnp.bfloat16)
    return {"acts_in": acts_in, "cot_out": cot_out, "w_in": w_in, "w_out": w_out}


def reference(acts_in, cot_out, w_in, w_out):
    rows_in = acts_in.reshape(-1, TOKEN_BLOCK, MODEL_DIM)
    rows_cot = cot_out.reshape(-1, TOKEN_BLOCK, MODEL_DIM)

    def fwd_step(x_cur, layer_w):
        w_in_l, w_out_l = layer_w
        hidden = jnp.dot(x_cur, w_in_l, preferred_element_type=jnp.float32).astype(jnp.bfloat16)
        active = gelu_pair(hidden)[0]
        x_next = x_cur + jnp.dot(active, w_out_l, preferred_element_type=jnp.float32).astype(jnp.bfloat16)
        return x_next, (x_cur, hidden)

    def bwd_step(grad_x, layer_items):
        w_in_l, w_out_l, x_saved, hidden = layer_items
        active, gelu_slope = gelu_pair(hidden)
        grad_act = jnp.dot(grad_x, w_out_l.T, preferred_element_type=jnp.float32).astype(jnp.bfloat16)
        grad_hid = (grad_act.astype(jnp.float32) * gelu_slope).astype(jnp.bfloat16)
        part_out = jnp.dot(active.T, grad_x, preferred_element_type=jnp.float32)
        part_in = jnp.dot(x_saved.T, grad_hid, preferred_element_type=jnp.float32)
        grad_prev = (grad_x.astype(jnp.float32) + jnp.dot(grad_hid, w_in_l.T, preferred_element_type=jnp.float32)).astype(jnp.bfloat16)
        return grad_prev, (part_in, part_out)

    def block_grads(acc_pair, block_pair):
        acc_in, acc_out = acc_pair
        x_first, grad_top = block_pair
        unused_top, saved_acts = lax.scan(fwd_step, x_first, (w_in, w_out))
        unused_bottom, layer_parts = lax.scan(bwd_step, grad_top, (w_in, w_out, saved_acts[0], saved_acts[1]), reverse=True)
        return (acc_in + layer_parts[0], acc_out + layer_parts[1]), None

    zero_acc = (jnp.zeros(w_in.shape, jnp.float32), jnp.zeros(w_out.shape, jnp.float32))
    final_acc, unused_ys = lax.scan(block_grads, zero_acc, (rows_in, rows_cot))
    return final_acc[0], final_acc[1]
```

```python
import functools
import math
import jax
import jax.numpy as jnp
from jax import lax
from jax.experimental import pallas as pl
from jax.experimental.layout import Layout, with_layout_constraint
from jax.experimental.pallas import tpu as pltpu
from jax.sharding import PartitionSpec as P

GROUP_AXIS = "fsdp"
BF, F32 = jnp.bfloat16, jnp.float32
C0 = math.sqrt(2.0 / math.pi)
C1 = C0 * 0.044715
VMEM_LIMIT = 67043328
ROW_BLOCK = 64


def dot(a, b):
    return jnp.dot(a, b, preferred_element_type=F32)


def dot_bt(a, b):
    return lax.dot_general(a, b, (((1,), (1,)), ((), ())), preferred_element_type=F32)


def gelu_value(hidden):
    u = hidden.astype(F32)
    t = jnp.tanh(u * (C1 * (u * u) + C0))
    return (0.5 * u * (1.0 + t)).astype(BF)


def gelu_pair(hidden):
    u = hidden.astype(F32)
    m = u * u
    t = jnp.tanh(u * (C1 * m + C0))
    s = 0.5 + 0.5 * t
    a = u * s
    slope = s + a * ((1.0 - t) * (3.0 * C1 * m + C0))
    return a.astype(BF), slope


def rows_of(width, tile):
    return pl.BlockSpec((tile, width), lambda i: (i, 0))


def resident(shape):
    return pl.BlockSpec(shape, lambda i: (0,) * len(shape), pipeline_mode=pl.Buffered(1))


def call(kernel, name, macs, **kw):
    return pl.pallas_call(
        kernel,
        name=name,
        compiler_params=pltpu.CompilerParams(vmem_limit_bytes=VMEM_LIMIT, dimension_semantics=("arbitrary",)),
        cost_estimate=pl.CostEstimate(flops=2 * macs, bytes_accessed=1 << 20, transcendentals=0),
        **kw,
    )


def hidden_kernel(x_ref, w_ref, h_ref):
    h_ref[...] = dot(x_ref[...], w_ref[...]).astype(BF)


def hidden_of(x, w, tile):
    tokens, width = x.shape
    hid = w.shape[1]
    return call(
        hidden_kernel, "hidden", tokens * width * hid,
        grid=(tokens // tile,),
        in_specs=[rows_of(width, tile), resident(w.shape)],
        out_specs=rows_of(hid, tile),
        out_shape=jax.ShapeDtypeStruct((tokens, hid), BF),
    )(x, w)


def part_rows(w_ref, lo, up, start, block):
    wide = up - lo
    pieces = []
    while block:
        owner, skip = divmod(start, wide)
        take = min(wide - skip, block)
        pieces.append(w_ref[owner, pl.ds(lo + skip, take), :])
        start, block = start + take, block - take
    return pieces[0] if len(pieces) == 1 else jnp.concatenate(pieces, 0)


def residual_kernel(tile, block, parts, x_ref, h_ref, w_ref, y_ref, total_scr):
    owners = w_ref.shape[0]
    base = 0
    for lo, up in parts:
        hid = owners * (up - lo)
        for c in range(hid // block):
            cols = pl.ds(base + c * block, block)
            active = jnp.concatenate(
                [gelu_value(h_ref[pl.ds(r * ROW_BLOCK, ROW_BLOCK), cols]) for r in range(tile // ROW_BLOCK)], 0)
            part = dot(active, part_rows(w_ref, lo, up, c * block, block))
            if base + c == 0:
                total_scr[...] = part
            else:
                total_scr[...] += part
        base += hid
    y_ref[...] = x_ref[...] + total_scr[...].astype(BF)


def residual_of(x, h, w, parts, tile, block):
    tokens, width = x.shape
    hid = h.shape[1]
    return call(
        functools.partial(residual_kernel, tile, block, parts), "residual", tokens * width * hid,
        grid=(tokens // tile,),
        in_specs=[rows_of(width, tile), rows_of(hid, tile), resident(w.shape)],
        out_specs=rows_of(width, tile),
        out_shape=jax.ShapeDtypeStruct(x.shape, BF),
        scratch_shapes=[pltpu.VMEM((tile, width), F32)],
    )(x, h, w)


def row_blocks(value):
    return [value[r:r + ROW_BLOCK] for r in range(0, value.shape[0], ROW_BLOCK)]


def hidden_grads(h_blocks, da, cols, dh_scr):
    actives, grads = [], []
    for r, (h, da_rows) in enumerate(zip(h_blocks, row_blocks(da))):
        active, slope = gelu_pair(h)
        grad = (da_rows.astype(F32) * slope).astype(BF)
        if dh_scr is not None:
            dh_scr[pl.ds(r * ROW_BLOCK, ROW_BLOCK), cols] = grad
        actives.append(active)
        grads.append(grad)
    return jnp.concatenate(actives, 0), jnp.concatenate(grads, 0)


def add_grads(active, grad, x_t, e_t, cols, g_in_acc, g_out_acc):
    g_out_acc[:, cols] += dot(e_t, active)
    grad_in = dot(x_t, grad)
    g_in_acc[:, :, cols] += grad_in.reshape(g_in_acc.shape[0], g_in_acc.shape[1], grad_in.shape[1])


def pipelined(n, first, second):
    ready = first(0)
    for c in range(n):
        following = first(c + 1) if c + 1 < n else None
        second(c, ready)
        ready = following


def clear(*accs):
    @pl.when(pl.program_id(0) == 0)
    def _():
        for acc in accs:
            acc[...] = jnp.zeros_like(acc)


def flush(g_in_acc, g_out_acc, grads_out, sems):
    owners, rows, hid = g_in_acc.shape
    own = hid // owners

    @pl.when(pl.program_id(0) == pl.num_programs(0) - 1)
    def _():
        copies = []
        for d in range(owners):
            cols = pl.ds(d * own, own)
            copies.append(pltpu.make_async_copy(g_out_acc.at[:, cols], grads_out.at[d, 0], sems.at[d]))
            copies.append(pltpu.make_async_copy(
                g_in_acc.at[:, :, cols], grads_out.at[:, 1, pl.ds(d * rows, rows), :], sems.at[owners + d]))
        for copy in copies:
            copy.start()
        for copy in copies:
            copy.wait()


def grad_shapes(width, hid, owners):
    out = jax.ShapeDtypeStruct((owners, 2, width, hid // owners), F32)
    scratch = [
        pltpu.VMEM((owners, width // owners, hid), F32),
        pltpu.VMEM((width, hid), F32),
        pltpu.SemaphoreType.DMA((2 * owners,)),
    ]
    return out, scratch


def top_kernel(tile, block, x_ref, e_ref, w1_ref, w2_ref, e_out, grads_out, g_in_acc, g_out_acc, sems, dh_scr):
    clear(g_in_acc, g_out_acc)
    x, e = x_ref[...], e_ref[...]
    x_t, e_t = x.T, e.T

    def first(c):
        cols = pl.ds(c * block, block)
        h = dot(x, w1_ref[:, cols]).astype(BF)
        da = dot_bt(e, w2_ref[cols, :]).astype(BF)
        return hidden_grads(row_blocks(h), da, cols, dh_scr)

    def second(c, ready):
        add_grads(*ready, x_t, e_t, pl.ds(c * block, block), g_in_acc, g_out_acc)

    pipelined(w1_ref.shape[1] // block, first, second)
    e_out[...] = (e.astype(F32) + dot_bt(dh_scr[...], w1_ref[...])).astype(BF)
    flush(g_in_acc, g_out_acc, grads_out, sems)


def top_layer(x, e, w1, w2, owners, tile, block):
    tokens, width = x.shape
    hid = w1.shape[1]
    out, scratch = grad_shapes(width, hid, owners)
    return call(
        functools.partial(top_kernel, tile, block), "top_layer", 5 * tokens * width * hid,
        grid=(tokens // tile,),
        in_specs=[rows_of(width, tile), rows_of(width, tile), resident(w1.shape), resident(w2.shape)],
        out_specs=[rows_of(width, tile), pl.BlockSpec(memory_space=pl.ANY)],
        out_shape=[jax.ShapeDtypeStruct(x.shape, BF), out],
        scratch_shapes=scratch + [pltpu.VMEM((tile, hid), BF)],
        input_output_aliases={0: 0},
    )(x, e, w1, w2)


def bottom_kernel(tile, block, part, x_ref, e_ref, h_ref, w2_ref, grads_out, g_in_acc, g_out_acc, sems):
    clear(g_in_acc, g_out_acc)
    e = e_ref[...]
    x_t, e_t = x_ref[...].T, e.T

    def first(c):
        cols = pl.ds(c * block, block)
        da = dot_bt(e, part_rows(w2_ref, *part, c * block, block)).astype(BF)
        h_blocks = [h_ref[pl.ds(r, ROW_BLOCK), cols] for r in range(0, tile, ROW_BLOCK)]
        return hidden_grads(h_blocks, da, cols, None)

    def second(c, ready):
        add_grads(*ready, x_t, e_t, pl.ds(c * block, block), g_in_acc, g_out_acc)

    pipelined(h_ref.shape[1] // block, first, second)
    flush(g_in_acc, g_out_acc, grads_out, sems)


def bottom_part(x, e, h, w2, part, first, tile, block):
    tokens, width = x.shape
    owners = w2.shape[0]
    hid = owners * (part[1] - part[0])
    out, scratch = grad_shapes(width, hid, owners)
    return call(
        functools.partial(bottom_kernel, tile, block, part), "bottom_part", 3 * tokens * width * hid,
        grid=(tokens // tile,),
        in_specs=[rows_of(width, tile), rows_of(width, tile), pl.BlockSpec((tile, hid), lambda i: (i, first // hid)), resident(w2.shape)],
        out_specs=pl.BlockSpec(memory_space=pl.ANY),
        out_shape=out,
        scratch_shapes=scratch,
    )(x, e, h, w2)


def part_columns_kernel(parts, owners, w_ref, out_ref):
    own = w_ref.shape[2] // owners
    base = 0
    for lo, up in parts:
        for d in range(owners):
            out_ref[:, pl.ds(base, up - lo)] = w_ref[0, :, pl.ds(d * own + lo, up - lo)]
            base += up - lo


def part_columns(w, parts, owners):
    _, rows, hid = w.shape
    return call(
        functools.partial(part_columns_kernel, parts, owners), "part_columns", rows * hid,
        grid=(1,),
        in_specs=[pl.BlockSpec((1, rows, hid), lambda i: (0, 0, 0))],
        out_specs=resident((rows, hid)),
        out_shape=jax.ShapeDtypeStruct((rows, hid), w.dtype),
    )(w)


def assemble_kernel(places, *refs):
    g_in, g_out = refs[-2:]
    _, rows, _ = g_in.shape
    _, own, width = g_out.shape
    for (layer, lo, up), ref in zip(places, refs):
        g_out[layer, pl.ds(lo, up - lo), :] = ref[pl.ds(0, width), :].T
        for d in range(width // rows):
            g_in[layer, :, pl.ds(d * own + lo, up - lo)] = ref[pl.ds(width + d * rows, rows), :]


def assemble(places, sums, rows, hid, own, width):
    shapes = ((2, rows, hid), (2, own, width))
    return call(
        functools.partial(assemble_kernel, places), "assemble", rows * hid,
        grid=(1,),
        in_specs=[resident(a.shape) for a in sums],
        out_specs=[resident(shape) for shape in shapes],
        out_shape=[jax.ShapeDtypeStruct(shape, F32) for shape in shapes],
    )(*sums)


def gather(rows):
    return lax.all_gather(rows, GROUP_AXIS, axis=0, tiled=True)


def scatter_sum(grads):
    total = lax.psum_scatter(grads.reshape(-1, grads.shape[-1]), GROUP_AXIS, scatter_dimension=0, tiled=True)
    return with_layout_constraint(total, Layout(major_to_minor=(0, 1)))


def solution(mesh):
    row_spec = P(None, GROUP_AXIS, None)
    owners = mesh.shape[GROUP_AXIS]

    def local_run(acts_loc, cot_loc, w_in_loc, w_out_loc):
        micro, tokens_loc, width = acts_loc.shape
        hid = w_in_loc.shape[2]
        rows, own = width // owners, hid // owners
        tokens = micro * tokens_loc
        x0 = acts_loc.reshape(tokens, width)
        e2 = cot_loc.reshape(tokens, width)

        parts = ((0, own - 128), (own - 128, own))
        w1 = gather(part_columns(w_in_loc, parts, owners))
        w1, first_out = lax.optimization_barrier((w1, w_out_loc[0]))
        w2 = gather(first_out)
        h0 = hidden_of(x0, w1, 1024)
        later_in, later_out, h0 = lax.optimization_barrier((w_in_loc[1], w_out_loc[1], h0))
        w1_top, w2_top = gather(later_in), gather(later_out)
        w2 = w2.reshape(owners, own, width)
        x1 = residual_of(x0, h0, w2, parts, 512, 1024)
        e1, top = top_layer(x1, e2, w1_top, w2_top, owners, 512, 1024)
        top = scatter_sum(top)
        large = scatter_sum(bottom_part(x0, e1, h0, w2, parts[0], 0, 1024, 512))
        e1, top = lax.optimization_barrier((e1, top))
        small = scatter_sum(bottom_part(x0, e1, h0, w2, parts[1], hid - owners * 128, 1024, 256))
        places = ((1, 0, own), (0, *parts[0]), (0, *parts[1]))
        return assemble(places, (top, large, small), rows, hid, own, width)

    return jax.shard_map(local_run, mesh=mesh, in_specs=(row_spec, row_spec, row_spec, row_spec), out_specs=(row_spec, row_spec), check_vma=False)
```

```python
import functools
import math
import jax
import jax.numpy as jnp
from jax import lax
from jax.experimental import pallas as pl
from jax.experimental.layout import Layout, with_layout_constraint
from jax.experimental.pallas import tpu as pltpu
from jax.sharding import PartitionSpec as P

GROUP_AXIS = "fsdp"
BF, F32 = jnp.bfloat16, jnp.float32
C0 = math.sqrt(2.0 / math.pi)
C1 = C0 * 0.044715
VMEM_LIMIT = 67043328
ROW_BLOCK = 64


def dot(a, b):
    return jnp.dot(a, b, preferred_element_type=F32)


def dot_bt(a, b):
    return lax.dot_general(a, b, (((1,), (1,)), ((), ())), preferred_element_type=F32)


def gelu_value(hidden):
    u = hidden.astype(F32)
    t = jnp.tanh(u * (C1 * (u * u) + C0))
    return (0.5 * u * (1.0 + t)).astype(BF)


def gelu_pair(hidden):
    u = hidden.astype(F32)
    m = u * u
    t = jnp.tanh(u * (C1 * m + C0))
    s = 0.5 + 0.5 * t
    a = u * s
    slope = s + a * ((1.0 - t) * (3.0 * C1 * m + C0))
    return a.astype(BF), slope


def rows_of(width, tile):
    return pl.BlockSpec((tile, width), lambda i: (i, 0))


def resident(shape):
    return pl.BlockSpec(shape, lambda i: (0,) * len(shape), pipeline_mode=pl.Buffered(1))


def call(kernel, name, macs, **kw):
    return pl.pallas_call(
        kernel,
        name=name,
        compiler_params=pltpu.CompilerParams(vmem_limit_bytes=VMEM_LIMIT, dimension_semantics=("arbitrary",)),
        cost_estimate=pl.CostEstimate(flops=2 * macs, bytes_accessed=1 << 20, transcendentals=0),
        **kw,
    )


def hidden_kernel(x_ref, w_ref, h_ref):
    h_ref[...] = dot(x_ref[...], w_ref[...]).astype(BF)


def hidden_of(x, w, tile):
    tokens, width = x.shape
    hid = w.shape[1]
    return call(
        hidden_kernel, "hidden", tokens * width * hid,
        grid=(tokens // tile,),
        in_specs=[rows_of(width, tile), resident(w.shape)],
        out_specs=rows_of(hid, tile),
        out_shape=jax.ShapeDtypeStruct((tokens, hid), BF),
    )(x, w)


def part_rows(w_ref, lo, up, start, block):
    wide = up - lo
    pieces = []
    while block:
        owner, skip = divmod(start, wide)
        take = min(wide - skip, block)
        pieces.append(w_ref[owner, pl.ds(lo + skip, take), :])
        start, block = start + take, block - take
    return pieces[0] if len(pieces) == 1 else jnp.concatenate(pieces, 0)


def residual_kernel(tile, block, parts, x_ref, *refs):
    h_refs = refs[:len(parts)]
    w_ref, y_ref, total_scr = refs[len(parts):]
    owners = w_ref.shape[0]
    fresh = True
    for h_ref, (lo, up) in zip(h_refs, parts):
        for c in range(owners * (up - lo) // block):
            cols = pl.ds(c * block, block)
            active = jnp.concatenate(
                [gelu_value(h_ref[pl.ds(r * ROW_BLOCK, ROW_BLOCK), cols]) for r in range(tile // ROW_BLOCK)], 0)
            part = dot(active, part_rows(w_ref, lo, up, c * block, block))
            if fresh:
                total_scr[...] = part
            else:
                total_scr[...] += part
            fresh = False
    y_ref[...] = x_ref[...] + total_scr[...].astype(BF)


def residual_of(x, h_parts, w, parts, tile, block):
    tokens, width = x.shape
    return call(
        functools.partial(residual_kernel, tile, block, parts), "residual", tokens * width * w.shape[0] * w.shape[1],
        grid=(tokens // tile,),
        in_specs=[rows_of(width, tile)] + [rows_of(h.shape[1], tile) for h in h_parts] + [resident(w.shape)],
        out_specs=rows_of(width, tile),
        out_shape=jax.ShapeDtypeStruct(x.shape, BF),
        scratch_shapes=[pltpu.VMEM((tile, width), F32)],
    )(x, *h_parts, w)


def row_blocks(value):
    return [value[r:r + ROW_BLOCK] for r in range(0, value.shape[0], ROW_BLOCK)]


def hidden_grads(h_blocks, da, cols, dh_scr):
    actives, grads = [], []
    for r, (h, da_rows) in enumerate(zip(h_blocks, row_blocks(da))):
        active, slope = gelu_pair(h)
        grad = (da_rows.astype(F32) * slope).astype(BF)
        if dh_scr is not None:
            dh_scr[pl.ds(r * ROW_BLOCK, ROW_BLOCK), cols] = grad
        actives.append(active)
        grads.append(grad)
    return jnp.concatenate(actives, 0), jnp.concatenate(grads, 0)


def add_grads(active, grad, x_t, e_t, cols, g_in_acc, g_out_acc):
    g_out_acc[:, cols] += dot(e_t, active)
    grad_in = dot(x_t, grad)
    g_in_acc[:, :, cols] += grad_in.reshape(g_in_acc.shape[0], g_in_acc.shape[1], grad_in.shape[1])


def pipelined(n, first, second):
    ready = first(0)
    for c in range(n):
        following = first(c + 1) if c + 1 < n else None
        second(c, ready)
        ready = following


def clear(*accs):
    @pl.when(pl.program_id(0) == 0)
    def _():
        for acc in accs:
            acc[...] = jnp.zeros_like(acc)


def flush(g_in_acc, g_out_acc, grads_out, sems):
    owners, rows, hid = g_in_acc.shape
    own = hid // owners

    @pl.when(pl.program_id(0) == pl.num_programs(0) - 1)
    def _():
        copies = []
        for d in range(owners):
            cols = pl.ds(d * own, own)
            copies.append(pltpu.make_async_copy(g_out_acc.at[:, cols], grads_out.at[d, 0], sems.at[d]))
            copies.append(pltpu.make_async_copy(
                g_in_acc.at[:, :, cols], grads_out.at[:, 1, pl.ds(d * rows, rows), :], sems.at[owners + d]))
        for copy in copies:
            copy.start()
        for copy in copies:
            copy.wait()


def grad_shapes(width, hid, owners):
    out = jax.ShapeDtypeStruct((owners, 2, width, hid // owners), F32)
    scratch = [
        pltpu.VMEM((owners, width // owners, hid), F32),
        pltpu.VMEM((width, hid), F32),
        pltpu.SemaphoreType.DMA((2 * owners,)),
    ]
    return out, scratch


def top_kernel(tile, block, x_ref, e_ref, w1_ref, w2_ref, e_out, grads_out, g_in_acc, g_out_acc, sems, dh_scr):
    clear(g_in_acc, g_out_acc)
    x, e = x_ref[...], e_ref[...]
    x_t, e_t = x.T, e.T

    def first(c):
        cols = pl.ds(c * block, block)
        h = dot(x, w1_ref[:, cols]).astype(BF)
        da = dot_bt(e, w2_ref[cols, :]).astype(BF)
        return hidden_grads(row_blocks(h), da, cols, dh_scr)

    def second(c, ready):
        add_grads(*ready, x_t, e_t, pl.ds(c * block, block), g_in_acc, g_out_acc)

    pipelined(w1_ref.shape[1] // block, first, second)
    e_out[...] = (e.astype(F32) + dot_bt(dh_scr[...], w1_ref[...])).astype(BF)
    flush(g_in_acc, g_out_acc, grads_out, sems)


def top_layer(x, e, w1, w2, owners, tile, block):
    tokens, width = x.shape
    hid = w1.shape[1]
    out, scratch = grad_shapes(width, hid, owners)
    return call(
        functools.partial(top_kernel, tile, block), "top_layer", 5 * tokens * width * hid,
        grid=(tokens // tile,),
        in_specs=[rows_of(width, tile), rows_of(width, tile), resident(w1.shape), resident(w2.shape)],
        out_specs=[rows_of(width, tile), pl.BlockSpec(memory_space=pl.ANY)],
        out_shape=[jax.ShapeDtypeStruct(x.shape, BF), out],
        scratch_shapes=scratch + [pltpu.VMEM((tile, hid), BF)],
        input_output_aliases={0: 0},
    )(x, e, w1, w2)


def bottom_kernel(tile, block, part, x_ref, e_ref, h_ref, w2_ref, grads_out, g_in_acc, g_out_acc, sems):
    clear(g_in_acc, g_out_acc)
    e = e_ref[...]
    x_t, e_t = x_ref[...].T, e.T

    def first(c):
        cols = pl.ds(c * block, block)
        da = dot_bt(e, part_rows(w2_ref, *part, c * block, block)).astype(BF)
        h_blocks = [h_ref[pl.ds(r, ROW_BLOCK), cols] for r in range(0, tile, ROW_BLOCK)]
        return hidden_grads(h_blocks, da, cols, None)

    def second(c, ready):
        add_grads(*ready, x_t, e_t, pl.ds(c * block, block), g_in_acc, g_out_acc)

    pipelined(h_ref.shape[1] // block, first, second)
    flush(g_in_acc, g_out_acc, grads_out, sems)


def bottom_part(x, e, h, w2, part, tile, block):
    tokens, width = x.shape
    owners = w2.shape[0]
    hid = owners * (part[1] - part[0])
    out, scratch = grad_shapes(width, hid, owners)
    return call(
        functools.partial(bottom_kernel, tile, block, part), "bottom_part", 3 * tokens * width * hid,
        grid=(tokens // tile,),
        in_specs=[rows_of(width, tile), rows_of(width, tile), rows_of(hid, tile), resident(w2.shape)],
        out_specs=pl.BlockSpec(memory_space=pl.ANY),
        out_shape=out,
        scratch_shapes=scratch,
    )(x, e, h, w2)


def part_columns_kernel(parts, owners, w_ref, *out_refs):
    own = w_ref.shape[2] // owners
    for out_ref, (lo, up) in zip(out_refs, parts):
        for d in range(owners):
            out_ref[:, pl.ds(d * (up - lo), up - lo)] = w_ref[0, :, pl.ds(d * own + lo, up - lo)]


def part_columns(w, parts, owners):
    _, rows, hid = w.shape
    widths = [owners * (up - lo) for lo, up in parts]
    return call(
        functools.partial(part_columns_kernel, parts, owners), "part_columns", rows * hid,
        grid=(1,),
        in_specs=[pl.BlockSpec((1, rows, hid), lambda i: (0, 0, 0))],
        out_specs=[resident((rows, wide)) for wide in widths],
        out_shape=[jax.ShapeDtypeStruct((rows, wide), w.dtype) for wide in widths],
    )(w)


def assemble_kernel(places, *refs):
    g_in, g_out = refs[-2:]
    _, rows, _ = g_in.shape
    _, own, width = g_out.shape
    for (layer, lo, up), ref in zip(places, refs):
        g_out[layer, pl.ds(lo, up - lo), :] = ref[pl.ds(0, width), :].T
        for d in range(width // rows):
            g_in[layer, :, pl.ds(d * own + lo, up - lo)] = ref[pl.ds(width + d * rows, rows), :]


def assemble(places, sums, rows, hid, own, width):
    shapes = ((2, rows, hid), (2, own, width))
    return call(
        functools.partial(assemble_kernel, places), "assemble", rows * hid,
        grid=(1,),
        in_specs=[resident(a.shape) for a in sums],
        out_specs=[resident(shape) for shape in shapes],
        out_shape=[jax.ShapeDtypeStruct(shape, F32) for shape in shapes],
    )(*sums)


def gather(rows):
    return lax.all_gather(rows, GROUP_AXIS, axis=0, tiled=True)


def scatter_sum(grads):
    total = lax.psum_scatter(grads.reshape(-1, grads.shape[-1]), GROUP_AXIS, scatter_dimension=0, tiled=True)
    return with_layout_constraint(total, Layout(major_to_minor=(0, 1)))


def solution(mesh):
    row_spec = P(None, GROUP_AXIS, None)
    owners = mesh.shape[GROUP_AXIS]

    def local_run(acts_loc, cot_loc, w_in_loc, w_out_loc):
        micro, tokens_loc, width = acts_loc.shape
        hid = w_in_loc.shape[2]
        rows, own = width // owners, hid // owners
        tokens = micro * tokens_loc
        x0 = acts_loc.reshape(tokens, width)
        e2 = cot_loc.reshape(tokens, width)

        parts = ((0, own - 128), (own - 128, own))
        w1_large, w1_small = part_columns(w_in_loc, parts, owners)
        w1_small, w1_large = lax.optimization_barrier((gather(w1_small), w1_large))
        w1_large = gather(w1_large)
        h_small = hidden_of(x0, w1_small, 2048)
        w1_large, first_out, h_small = lax.optimization_barrier((w1_large, w_out_loc[0], h_small))
        w2 = gather(first_out).reshape(owners, own, width)
        h_large = hidden_of(x0, w1_large, 1024)
        later_in, later_out, h_large = lax.optimization_barrier((w_in_loc[1], w_out_loc[1], h_large))
        w1_top, w2_top = gather(later_in), gather(later_out)
        x1 = residual_of(x0, (h_large, h_small), w2, parts, 512, 1024)
        e1, top = top_layer(x1, e2, w1_top, w2_top, owners, 512, 1536)
        top = scatter_sum(top)
        large = scatter_sum(bottom_part(x0, e1, h_large, w2, parts[0], 1024, 512))
        e1, top = lax.optimization_barrier((e1, top))
        small = scatter_sum(bottom_part(x0, e1, h_small, w2, parts[1], 1024, 256))
        places = ((1, 0, own), (0, *parts[0]), (0, *parts[1]))
        return assemble(places, (top, large, small), rows, hid, own, width)

    return jax.shard_map(local_run, mesh=mesh, in_specs=(row_spec, row_spec, row_spec, row_spec), out_specs=(row_spec, row_spec), check_vma=False)
```
